256 devices in a mesh: dp: 64 (over z_lo, x, y, core), vocab: 4 (over z_hi).
Axes of the slice: x: 4, y: 4, z: 8 (z_hi: 4, z_lo: 2; z = z_hi * 2 + z_lo), core: 2. Of those that a mesh axis runs over, the one named last changes fastest.
Arguments:
- hidden: bfloat16 [512, 4096], P('dp'), may hold values from -16 to 16
- embed_grad: bfloat16 [512, 4096], P('dp'), may hold values from -8 to 8
- token_ids: int32 [512], P('dp'), may hold values from 0 to 32767
- loss_weight: float32 [512], P('dp'), may hold values from 16 to 256
- teacher_logits: bfloat16 [512, 32768], P('dp', 'vocab'), may hold values from -24 to 256
- head: bfloat16 [4096, 32768], P('dp', 'vocab'), may hold values from -1 to 1
Outputs:
- grad_hidden: bfloat16 [512, 4096], P('dp', 'vocab')
- head_grad: float32 [4096, 32768], P('dp', 'vocab')
The draws below stay inside these ranges and needn't reach their ends.
Inputs may be any that keep to these rules, and one draw needn't show every extreme that they name: `token_ids`: token ids of the vocabulary window.
All inputs are finite; a program needn't handle non-finite values.
Results may differ from the reference program's by a relative error of at most 0.0022.
The reference program's roundings to bfloat16 on the way (of `gap`) count: a program that leaves them out, or rounds other values in their place, can miss the bound.
Values may be sent and summed in bfloat16 or wider, within the bound.
No kernel may reach another device: no remote copies, remote signals or barrier semaphores. Data moves between devices by JAX's collectives and lax.ppermute only.
A program may use at most 128 MiB of HBM per device.

```python
import math
import jax
import jax.numpy as jnp
import numpy as np
from jax import lax

D = 4096
TOKENS = 512
VOCAB_WIN = 32768


def head_values(key):
    raw = jax.random.normal(jax.random.fold_in(key, 11), (D, VOCAB_WIN), jnp.float32)
    return jnp.clip(raw * (3.0 / math.sqrt(D)), -1.0, 1.0)


def draw_head(key, part):
    return head_values(key).astype(jnp.bfloat16)


def draw_hidden(key, part):
    base = jax.random.normal(jax.random.fold_in(key, 23), (TOKENS, D), jnp.float32)
    return jnp.clip(base, -16.0, 16.0).astype(jnp.bfloat16)


def draw_teacher_logits(key, part):
    base = jax.random.normal(jax.random.fold_in(key, 53), (TOKENS, VOCAB_WIN), jnp.float32) * 3.0
    return jnp.clip(base, -24.0, 256.0).astype(jnp.bfloat16)


def place_ends(values, stream_key, smallest, top_value):
    dims = values.shape
    index_at = [jax.random.randint(jax.random.fold_in(stream_key, axis), (), 0, dims[axis]) for axis in range(len(dims))]
    values = values.at[tuple(index_at)].set(smallest)
    longest = dims.index(max(dims))
    index_at[longest] = (index_at[longest] + 1) % dims[longest]
    return values.at[tuple(index_at)].set(top_value)


def with_spikes(result, rng, source, target, blocks, factor):
    def block_of(axis_at):
        return (jnp.arange(result.shape[axis_at]) // (result.shape[axis_at] // blocks)).reshape((-1,) + (1,) * (result.ndim - 1 - axis_at))

    one_side = jax.random.permutation(rng, blocks)[block_of(target)]
    second = (block_of(target) + blocks // 2) % blocks
    return jnp.where((block_of(source) == one_side) | (block_of(source) == second), factor * result, result)


def shard_levels(own_key, dims, split, low, top_value):
    factor_of, own = 1.0, jax.random.fold_in(own_key, 6)
    for dim, blocks in split:
        heights = jnp.exp(jax.random.uniform(jax.random.fold_in(own, dim), (blocks,), jnp.float32, low / len(split), top_value / len(split)))
        factor_of = factor_of * jnp.repeat(heights, dims[dim] // blocks).reshape([-1 if axis == dim else 1 for axis in range(len(dims))])
    return factor_of


def cumulative_ranks(amount, lean):
    loads = [(1 << 20) // math.isqrt(grade ** lean) + 1 for grade in range(1, amount + 1)]
    width = 1 + sum(loads) // (1 << 30)
    return np.cumsum(np.array([max(1, weight // width) for weight in loads]))


def ranked_ids(stream_key, dims, amount, slope):
    table = cumulative_ranks(amount, slope)
    ticket = jax.random.randint(jax.random.fold_in(stream_key, 1), dims, 0, int(table[amount - 1]))
    rank = jnp.searchsorted(jnp.asarray(table, jnp.int32), ticket, side="right")
    return jax.random.permutation(jax.random.fold_in(stream_key, 2), amount)[rank].astype(jnp.int32)


def bell_draw_with(key, extent, deviation, most, shards, heavy, kind=jnp.bfloat16):
    drawn = deviation * jax.random.normal(key, extent, jnp.float32)
    if shards:
        drawn = drawn * shard_levels(key, extent, shards, -0.22, 0.18)
    return jnp.clip(with_spikes(drawn, jax.random.fold_in(key, 3), *heavy), -most, most).astype(kind)


def setup_inputs(seed: int = 0) -> dict:
    streams_of = jax.random.split(jax.random.key(seed), 7)
    return {
        "hidden": draw_hidden(jax.random.fold_in(streams_of[6], 71), 0),
        "embed_grad": bell_draw_with(streams_of[1], (TOKENS, D), 0.5, 8.0, ((0, 64),), (0, 1, 64, 4.0)),
        "token_ids": place_ends(ranked_ids(streams_of[2], (TOKENS,), VOCAB_WIN, 2), jax.random.fold_in(streams_of[2], 3), 0, VOCAB_WIN - 1).astype(jnp.int32),
        "loss_weight": jnp.clip(jnp.exp(math.log(256.0) - 2.7725887 * jax.random.uniform(streams_of[3], (TOKENS,), jnp.float32) ** shard_levels(streams_of[3], (TOKENS,), ((0, 64),), -0.2, 0.2)), 16.0, 256.0),
        "teacher_logits": draw_teacher_logits(jax.random.fold_in(streams_of[6], 71), 0),
        "head": draw_head(jax.random.fold_in(streams_of[6], 71), 0),
    }


def reference(hidden, embed_grad, token_ids, loss_weight, teacher_logits, head):
    student = jnp.dot(hidden, head, preferred_element_type=jnp.float32)
    teacher = teacher_logits.astype(jnp.float32)
    student_norm = jax.nn.logsumexp(student, axis=1, keepdims=True)
    teacher_norm = jax.nn.logsumexp(teacher, axis=1, keepdims=True)
    gap = (loss_weight[:, None] * (jnp.exp(student - student_norm) - jnp.exp(teacher - teacher_norm))).astype(jnp.bfloat16)
    dense_part = lax.dot_general(hidden, gap, (((0,), (0,)), ((), ())), preferred_element_type=jnp.float32)
    head_grad = dense_part.at[:, token_ids.astype(jnp.int32)].add(embed_grad.astype(jnp.float32).T)
    grad_hidden = lax.dot_general(gap, head, (((1,), (1,)), ((), ())), preferred_element_type=jnp.float32).astype(jnp.bfloat16)
    return grad_hidden, head_grad
```

```python
import jax
import jax.numpy as jnp
from jax import lax
from jax.sharding import Mesh
from jax.sharding import PartitionSpec as P

DP = ("z", "x", "y", "c")
COLS = ("z", "x", "c")


def exchange(x, axes):
    return lax.all_to_all(x, axes, 0, 0, tiled=True)


def in_pieces(x, count):
    pieces = []
    for _ in range(count):
        piece = lax.reduce_precision(x, 8, 7)
        pieces.append(piece.astype(jnp.bfloat16))
        x = x - piece
    return jnp.stack(pieces, axis=-1)


def dot(left, right, contract):
    return lax.dot_general(left, right, (contract, ((), ())), preferred_element_type=jnp.float32)


def per_device(hidden, embed_grad, token_ids, loss_weight, teacher_logits, head):
    bf16, f32 = jnp.bfloat16, jnp.float32
    sizes = {axis: lax.axis_size(axis) for axis in DP + ("vocab",)}
    nz, nx, ny, nc, nv = (sizes[axis] for axis in DP + ("vocab",))
    own, width = hidden.shape
    rows, vocab = head.shape
    cols = nz * nx * nc
    devices = cols * ny
    block = vocab // cols
    tokens = devices * own
    part = cols * rows

    hidden_out = hidden.reshape(own, nz * nx, ny, nc * rows)
    hidden_out = hidden_out.transpose(2, 0, 1, 3).reshape(ny, 1, own, part)
    hidden_out = jnp.broadcast_to(hidden_out, (ny, cols, own, part)).reshape(devices, own, part)
    embed_out = embed_grad.reshape(own, nz * nx, ny, nc, rows)
    embed_out = embed_out.transpose(2, 1, 3, 0, 4).reshape(devices, own, rows)
    id_high = token_ids // 256
    extra = jnp.concatenate(
        [
            id_high[:, None].astype(bf16),
            (token_ids - 256 * id_high)[:, None].astype(bf16),
            in_pieces(loss_weight, 3),
        ],
        axis=1,
    )
    extra = jnp.pad(extra, ((0, 0), (0, 128 - rows - extra.shape[1])))
    extra = jnp.broadcast_to(extra[None], (devices, *extra.shape))
    sent = jnp.concatenate([hidden_out, embed_out, extra], axis=2)
    mine = exchange(sent, ("y", "z", "x", "c")).reshape(tokens, part + 128)
    hidden_part = mine[:, :part]
    embed_cols = mine[:, part : part + rows]
    ids = mine[:, part + rows : part + rows + 2].astype(jnp.int32)
    ids = ids[:, 0] * 256 + ids[:, 1]
    weights = mine[:, part + rows + 2 : part + rows + 5].astype(f32)
    weights = weights[:, 0] + weights[:, 1] + weights[:, 2]
    weights = lax.dynamic_index_in_dim(
        weights.reshape(ny, cols * own), lax.axis_index("y"), 0, keepdims=False
    )

    stacked = jnp.concatenate([head, teacher_logits], axis=0).reshape(rows + own, cols, block)
    stacked = exchange(stacked.swapaxes(0, 1), COLS)
    head_part = stacked[:, :rows].reshape(part, block)
    teacher = stacked[:, rows:].reshape(cols * own, block).astype(f32)

    student = dot(hidden_part, head_part, ((1,), (0,))).reshape(ny, cols * own, block)
    student = exchange(student, "y").sum(axis=0)

    student_max = jnp.max(student, axis=1)
    teacher_max = jnp.max(teacher, axis=1)
    student_sum = jnp.sum(jnp.exp(student - student_max[:, None]), axis=1)
    teacher_sum = jnp.sum(jnp.exp(teacher - teacher_max[:, None]), axis=1)
    stats = jnp.stack([student_max, teacher_max, student_sum, teacher_sum])
    stats = exchange(
        jnp.broadcast_to(stats[None], (cols * nv, *stats.shape)), COLS + ("vocab",)
    )
    tops = jnp.max(stats[:, :2], axis=0)
    totals = jnp.sum(stats[:, 2:] * jnp.exp(stats[:, :2] - tops), axis=0)
    norms = tops + jnp.log(totals)
    gap = (
        weights[:, None]
        * (jnp.exp(student - norms[0][:, None]) - jnp.exp(teacher - norms[1][:, None]))
    ).astype(bf16)
    gap = exchange(jnp.broadcast_to(gap[None], (ny, *gap.shape)), "y")

    gap_rows = gap.reshape(tokens, block)
    gap_by_core = gap.reshape(ny, nz * nx, nc, own, block).transpose(2, 1, 0, 3, 4)
    back = dot(gap_by_core.reshape(tokens, block), head_part, ((1,), (1,)))
    back = exchange(back.reshape(nc, tokens // nc, part), "c").sum(axis=0)
    back = exchange(back.reshape(nz * nx, ny * own, part), ("z", "x")).sum(axis=0)
    back = back.reshape(ny, own, nv, part // nv).transpose(0, 2, 1, 3)
    back = exchange(back.reshape(ny * nv, own, part // nv), ("y", "vocab"))
    back = back.reshape(ny, nv, own, part // nv).sum(axis=1)
    back = back.reshape(ny, own, part // nv // (nc * rows), nc * rows).transpose(1, 2, 0, 3)
    grad_hidden = back.reshape(own, width // nv).astype(bf16)

    dense = dot(hidden_part, gap_rows, ((0,), (0,))).astype(bf16)
    dense = exchange(dense.reshape(cols, rows, block), COLS)
    dense = dense.swapaxes(0, 1).reshape(rows, vocab)
    vocab_ids = lax.axis_index("vocab") * vocab + jnp.arange(vocab, dtype=jnp.int32)
    lookup = (ids[:, None] == vocab_ids[None, :]).astype(bf16)
    head_grad = dot(embed_cols, lookup, ((0,), (0,))) + dense.astype(f32)
    return grad_hidden, head_grad


def solution(mesh):
    torus = Mesh(
        mesh.devices.reshape(2, 4, 4, 2, mesh.shape["vocab"]), ("z", "x", "y", "c", "vocab")
    )
    in_specs = (P(DP, None), P(DP, None), P(DP), P(DP), P(DP, "vocab"), P(DP, "vocab"))
    out_specs = (P(DP, "vocab"), P(DP, "vocab"))
    return jax.shard_map(
        per_device, mesh=torus, in_specs=in_specs, out_specs=out_specs, check_vma=False
    )
```

```python
import functools

import jax
import jax.numpy as jnp
from jax import lax
from jax.experimental import pallas as pl
from jax.experimental.pallas import tpu as pltpu
from jax.sharding import Mesh
from jax.sharding import PartitionSpec as P


DP = ("z", "x", "y", "c")
COLS = ("z", "x", "c")
FIT = 64.0
SMEM = pl.BlockSpec(memory_space=pltpu.SMEM)
VMEM = pl.BlockSpec(memory_space=pltpu.VMEM)


def exchange(x, axes):
    return lax.all_to_all(x, axes, 0, 0, tiled=True)


def shifted(x, axis, step):
    size = lax.axis_size(axis)
    return lax.ppermute(x, axis, [(k, (k + step) % size) for k in range(size)])


def shifted_both(x, z_step, x_step):
    nz, nx = lax.axis_size("z"), lax.axis_size("x")
    pairs = [
        (z * nx + k, (z + z_step) % nz * nx + (k + x_step) % nx)
        for z in range(nz)
        for k in range(nx)
    ]
    return lax.ppermute(x, ("z", "x"), pairs)


def in_pieces(x, count):
    pieces = []
    for _ in range(count):
        piece = lax.reduce_precision(x, 8, 7)
        pieces.append(piece.astype(jnp.bfloat16))
        x = x - piece
    return jnp.stack(pieces, axis=-1)


def dot(left, right, contract):
    return lax.dot_general(left, right, (contract, ((), ())), preferred_element_type=jnp.float32)


def split_kernel(place, hidden, *outs, groups, step):
    ny = len(outs)
    for k, out in enumerate(outs):
        to = lax.rem(place[2] + k, ny)
        for g in range(groups):
            out[:, g * step : (g + 1) * step] = hidden[
                :, pl.ds(pl.multiple_of((g * ny + to) * step, 128), step)
            ]


def row_of(place, sizes, dc, dx, dz):
    nz, nx, nc = sizes
    z = lax.rem(place[0] + (nz - dz), nz)
    x = lax.rem(place[1] + (nx - dx), nx)
    c = lax.rem(place[3] + (nc - dc), nc)
    return (z * nx + x) * nc + c


def student_kernel(place, same, other, head, *outs, sizes, own):
    nz, nx, nc = sizes
    ny = len(outs)
    for dc, half in enumerate((same, other)):
        made = jnp.dot(half[...], head[...], preferred_element_type=jnp.float32)
        at = 0
        for dx in range(nx):
            for dz in range(nz):
                row = pl.multiple_of(row_of(place, sizes, dc, dx, dz) * own, own)
                for k in range(ny):
                    outs[k][pl.ds(row, own), :] = made[at : at + own, :]
                    at += own


def back_kernel(place, g0, g1, g2, g3, head, same, other, gap, *, sizes, own):
    nz, nx, nc = sizes
    gaps = (g0, g1, g2, g3)
    at = 0
    for dc in range(nc):
        for dx in range(nx):
            for dz in range(nz):
                row = pl.multiple_of(row_of(place, sizes, dc, dx, dz) * own, own)
                for part in gaps:
                    gap[at : at + own, :] = part[pl.ds(row, own), :]
                    at += own
    half = at // nc
    for dc, out in ((1, other), (0, same)):
        out[...] = lax.dot_general(
            gap[dc * half : (dc + 1) * half, :],
            head[...],
            (((1,), (1,)), ((), ())),
            preferred_element_type=jnp.float32,
        )


def per_device(hidden, embed_grad, token_ids, loss_weight, teacher_logits, head):
    bf16, f32 = jnp.bfloat16, jnp.float32
    sizes = {axis: lax.axis_size(axis) for axis in DP + ("vocab",)}
    nz, nx, ny, nc, nv = (sizes[axis] for axis in DP + ("vocab",))
    own, width = hidden.shape
    rows, vocab = head.shape
    cols = nz * nx * nc
    devices = cols * ny
    block = vocab // cols
    tokens = devices * own
    part = cols * rows
    group = cols * own
    place = jnp.stack([lax.axis_index(axis) for axis in DP]).astype(jnp.int32)

    stacked = jnp.concatenate([head, teacher_logits], axis=0).reshape(rows + own, cols, block)
    stacked = exchange(stacked.swapaxes(0, 1), COLS)
    head_part = stacked[:, :rows].reshape(part, block)
    teacher = stacked[:, rows:].reshape(group, block).astype(f32)

    pieces = pl.pallas_call(
        functools.partial(split_kernel, groups=nz * nx, step=nc * rows),
        out_shape=[jax.ShapeDtypeStruct((own, part), bf16)] * ny,
        in_specs=[SMEM, VMEM],
        out_specs=[VMEM] * ny,
        name="split_hidden",
    )(place, hidden)
    line = jnp.concatenate(
        [pieces[0]] + [shifted(pieces[k], "y", k) for k in range(1, ny)], axis=0
    )
    line = jnp.concatenate([line, shifted(line, "z", 1)], axis=0)
    same = jnp.concatenate([line] + [shifted(line, "x", k) for k in range(1, nx)], axis=0)
    other = shifted(same, "c", 1)

    partials = list(pl.pallas_call(
        functools.partial(student_kernel, sizes=(nz, nx, nc), own=own),
        out_shape=[jax.ShapeDtypeStruct((group, block), f32)] * ny,
        in_specs=[SMEM] + [VMEM] * 3,
        out_specs=[VMEM] * ny,
        name="student_partials",
    )(place, same, other, head_part))
    student = partials[0]
    for k in range(1, ny):
        student = student + shifted(partials[k], "y", -k)

    embed_out = embed_grad.reshape(own, nz * nx, ny, nc, rows)
    embed_out = embed_out.transpose(2, 1, 3, 0, 4).reshape(devices, own, rows)
    id_high = token_ids // 256
    extra = jnp.concatenate(
        [
            id_high[:, None].astype(bf16),
            (token_ids - 256 * id_high)[:, None].astype(bf16),
            in_pieces(loss_weight, 3),
        ],
        axis=1,
    )
    extra = jnp.pad(extra, ((0, 0), (0, 128 - rows - extra.shape[1])))
    extra = jnp.broadcast_to(extra[None], (devices, *extra.shape))
    sent, partials[0] = lax.optimization_barrier(
        (jnp.concatenate([embed_out, extra], axis=2), partials[0])
    )
    mine = exchange(sent, ("y", "z", "x", "c")).reshape(tokens, 128)
    embed_cols = mine[:, :rows]
    ids = mine[:, rows : rows + 2].astype(jnp.int32)
    ids = ids[:, 0] * 256 + ids[:, 1]
    weights = mine[:, rows + 2 : rows + 5].astype(f32)
    weights = weights[:, 0] + weights[:, 1] + weights[:, 2]
    weights = lax.dynamic_index_in_dim(
        weights.reshape(ny, group), place[2], 0, keepdims=False
    )

    student_max = jnp.max(student, axis=1)
    teacher_max = jnp.max(teacher, axis=1)
    student_sum = jnp.sum(jnp.exp(student - student_max[:, None]), axis=1)
    teacher_sum = jnp.sum(jnp.exp(teacher - teacher_max[:, None]), axis=1)
    stats = jnp.stack(
        [student_max + jnp.log(student_sum), teacher_max + jnp.log(teacher_sum)]
    )
    stats = exchange(
        jnp.broadcast_to(stats[None], (cols * nv, *stats.shape)), COLS + ("vocab",)
    )
    tops = jnp.max(stats, axis=0)
    norms = tops + jnp.log(jnp.sum(jnp.exp(stats - tops), axis=0))
    gap = (
        weights[:, None]
        * (jnp.exp(student - norms[0][:, None]) - jnp.exp(teacher - norms[1][:, None]))
    ).astype(bf16)
    gaps = [gap] + [shifted(gap, "y", k) for k in range(1, ny)]

    half = tokens // nc
    back, back_other, gap_all = pl.pallas_call(
        functools.partial(back_kernel, sizes=(nz, nx, nc), own=own),
        out_shape=[
            jax.ShapeDtypeStruct((half, part), f32),
            jax.ShapeDtypeStruct((half, part), f32),
            jax.ShapeDtypeStruct((tokens, block), bf16),
        ],
        in_specs=[SMEM] + [VMEM] * 5,
        out_specs=[VMEM] * 3,
        name="hidden_back",
    )(place, *gaps, head_part)
    dense = dot(same, gap_all[:half], ((0,), (0,))) + dot(other, gap_all[half:], ((0,), (0,)))
    dense = exchange(dense.astype(bf16).reshape(cols, rows, block), COLS)

    back = back + shifted(back_other, "c", 1)
    back = back.reshape(nx, nz, ny * own, part)
    total = back[0, 0]
    sent = (back * FIT).astype(jnp.float16)
    for dx in range(nx):
        for dz in range(nz):
            if dx or dz:
                total = total + shifted_both(sent[dx, dz], dz, -dx).astype(f32) * (1 / FIT)
    total = total.reshape(ny, own, part)
    total = jnp.concatenate([total[:1], jnp.flip(total[1:], axis=0)], axis=0)
    total = jnp.roll(total, place[2], axis=0)
    total = total.reshape(ny, own, nv, part // nv).transpose(0, 2, 1, 3)
    total, dense = lax.optimization_barrier(
        (total.reshape(ny * nv, own, part // nv), dense)
    )
    total = exchange(total, ("y", "vocab"))
    total = total.reshape(ny, nv, own, part // nv).sum(axis=1)
    total = total.reshape(ny, own, part // nv // (nc * rows), nc * rows).transpose(1, 2, 0, 3)
    grad_hidden = total.reshape(own, width // nv).astype(bf16)

    dense = dense.swapaxes(0, 1).reshape(rows, vocab)
    vocab_ids = lax.axis_index("vocab") * vocab + jnp.arange(vocab, dtype=jnp.int32)
    lookup = (ids[:, None] == vocab_ids[None, :]).astype(bf16)
    head_grad = dot(embed_cols, lookup, ((0,), (0,))) + dense.astype(f32)
    return grad_hidden, head_grad


def solution(mesh):
    torus = Mesh(
        mesh.devices.reshape(2, 4, 4, 2, mesh.shape["vocab"]), ("z", "x", "y", "c", "vocab")
    )
    in_specs = (P(DP, None), P(DP, None), P(DP), P(DP), P(DP, "vocab"), P(DP, "vocab"))
    out_specs = (P(DP, "vocab"), P(DP, "vocab"))
    return jax.shard_map(
        per_device, mesh=torus, in_specs=in_specs, out_specs=out_specs, check_vma=False
    )
```

```python
import functools

import jax
import jax.numpy as jnp
from jax import lax
from jax.experimental import pallas as pl
from jax.experimental.pallas import tpu as pltpu
from jax.sharding import Mesh
from jax.sharding import PartitionSpec as P


DP = ("z", "x", "y", "c")
COLS = ("z", "x", "c")
FIT = 64.0
SMEM = pl.BlockSpec(memory_space=pltpu.SMEM)
VMEM = pl.BlockSpec(memory_space=pltpu.VMEM)
HBM = pl.BlockSpec(memory_space=pltpu.MemorySpace.HBM)


def exchange(x, axes):
    return lax.all_to_all(x, axes, 0, 0, tiled=True)


def shifted(x, axis, step):
    size = lax.axis_size(axis)
    return lax.ppermute(x, axis, [(k, (k + step) % size) for k in range(size)])


def shifted_both(x, z_step, x_step):
    nz, nx = lax.axis_size("z"), lax.axis_size("x")
    pairs = [
        (z * nx + k, (z + z_step) % nz * nx + (k + x_step) % nx)
        for z in range(nz)
        for k in range(nx)
    ]
    return lax.ppermute(x, ("z", "x"), pairs)


def dot(left, right, contract):
    return lax.dot_general(left, right, (contract, ((), ())), preferred_element_type=jnp.float32)


def call(body, outs, scratch=(), ins=None):
    def run(place, *operands):
        specs = list(ins or [VMEM] * len(operands))
        operands = [
            pltpu.with_memory_space_constraint(x, pltpu.MemorySpace.HBM) if spec is not VMEM else x
            for x, spec in zip(operands, specs)
        ]
        return pl.pallas_call(
            body,
            out_shape=[spec.memory_space(out.shape, out.dtype) for out, spec in outs],
            in_specs=[SMEM] + specs,
            out_specs=[spec for _, spec in outs],
            scratch_shapes=list(scratch),
            compiler_params=pltpu.CompilerParams(vmem_limit_bytes=16 << 20),
        )(place, *operands)

    return run


def held(shape, dtype):
    return jax.ShapeDtypeStruct(shape, dtype), VMEM


def stored(shape, dtype):
    return jax.ShapeDtypeStruct(shape, dtype), HBM


def joined(x):
    top = jnp.max(x, axis=0)
    return top + jnp.log(jnp.sum(jnp.exp(x - top), axis=0))


def position(place, sizes):
    _, nx, ny, nc, nv = sizes
    at = place[0] // nv
    c = lax.rem(at, nc)
    y = lax.rem(at // nc, ny)
    x = lax.rem(at // (nc * ny), nx)
    return at // (nc * ny * nx), x, y, c


def row_of(where, sizes, dc, dx, dz):
    nz, nx, _, nc, _ = sizes
    z = lax.rem(where[0] + (nz - dz), nz)
    x = lax.rem(where[1] + (nx - dx), nx)
    c = lax.rem(where[3] + (nc - dc), nc)
    return (z * nx + x) * nc + c


def send_kernel(place, ids, weights, hidden, embed, head, teacher, *refs, sizes):
    nz, nx, ny, _, _ = sizes
    stacked, outs = refs[0], refs[1 : 1 + ny]
    hidden_here, embed_here, sems = refs[1 + ny :]
    _, _, y, _ = position(place, sizes)
    rows, own = head.shape[0], teacher.shape[0]
    cols, _, block = stacked.shape
    step = hidden.shape[1] // (nz * nx * ny)
    moves = [(hidden, hidden_here), (embed, embed_here)]
    for j in range(cols):
        lanes = slice(j * block, (j + 1) * block)
        moves.append((head.at[:, lanes], stacked.at[j, :rows, :]))
        moves.append((teacher.at[:, lanes], stacked.at[j, rows : rows + own, :]))
    moves = [pltpu.make_async_copy(*move, sems.at[k]) for k, move in enumerate(moves)]
    for move in moves:
        move.start()
    line = lax.broadcasted_iota(jnp.int32, (own, 128), 0)
    lane = lax.broadcasted_iota(jnp.int32, (own, 128), 1)
    weight = jnp.zeros((own, 128), jnp.float32)
    number = jnp.zeros((own, 128), jnp.int32)
    for t in range(own):
        weight = jnp.where(line == t, weights[t], weight)
        number = jnp.where(line == t, ids[t], number)
    number = jnp.where(lane == rows, number // 256, lax.rem(number, 256))
    number = jnp.where((lane == rows) | (lane == rows + 1), number, 0)
    number = number.astype(jnp.float32).astype(jnp.bfloat16)
    for q in range(block // 128):
        piece = weight.astype(jnp.bfloat16)
        weight = weight - piece.astype(jnp.float32)
        for j in range(cols):
            stacked[j, rows + own :, q * 128 : (q + 1) * 128] = piece
    moves[0].wait()
    moves[1].wait()
    for k, out in enumerate(outs):
        to = lax.rem(y + k, ny)
        for g in range(nz * nx):
            lanes = pl.ds(pl.multiple_of((g * ny + to) * step, step), step)
            out[:, g * step : (g + 1) * step] = hidden_here[:, lanes]
            out[:, (nz * nx + g) * step : (nz * nx + g + 1) * step] = embed_here[:, lanes]
        out[:, 2 * nz * nx * step :] = number
    for move in moves[2:]:
        move.wait()


def student_kernel(place, same, other, stacked, *refs, sizes, own, rows):
    where = position(place, sizes)
    nz, nx, ny, nc, _ = sizes
    outs, kept, head, sem = refs[:ny], refs[ny], refs[ny + 1], refs[ny + 2]
    for j in range(nz * nx * nc):
        head[j * rows : (j + 1) * rows, :] = stacked[j, :rows, :]
    keep = pltpu.make_async_copy(head, kept, sem)
    keep.start()
    for dc, half in enumerate((same, other)):
        made = jnp.dot(half[...], head[...], preferred_element_type=jnp.float32)
        at = 0
        for dx in range(nx):
            for dz in range(nz):
                row = pl.multiple_of(row_of(where, sizes, dc, dx, dz) * own, own)
                for k in range(ny):
                    outs[k][pl.ds(row, own), :] = made[at : at + own, :]
                    at += own
    keep.wait()


def back_kernel(place, g0, g1, g2, g3, kept, same, other, gap, head, sem, *, sizes, own):
    where = position(place, sizes)
    nz, nx, _, nc, _ = sizes
    fetch = pltpu.make_async_copy(kept, head, sem)
    fetch.start()
    at = 0
    for dc in range(nc):
        for dx in range(nx):
            for dz in range(nz):
                row = pl.multiple_of(row_of(where, sizes, dc, dx, dz) * own, own)
                for part in (g0, g1, g2, g3):
                    gap[at : at + own, :] = part[pl.ds(row, own), :]
                    at += own
    half = at // nc
    fetch.wait()
    for dc, out in ((1, other), (0, same)):
        out[...] = lax.dot_general(
            gap[dc * half : (dc + 1) * half, :],
            head[...],
            (((1,), (1,)), ((), ())),
            preferred_element_type=jnp.float32,
        )


def arrange_kernel(place, *refs, sizes):
    _, _, ny, _, nv = sizes
    _, _, y, _ = position(place, sizes)
    v = lax.rem(place[0], nv)
    parts, outs = refs[:ny], refs[ny:]
    width = parts[0].shape[1] // nv
    for k, out in enumerate(outs):
        start = lax.rem(v + k, nv) * width
        for j, part in enumerate(parts):
            for g in range(width // 128):
                to = pl.multiple_of((g * ny + lax.rem(y + j, ny)) * 128, 128)
                out[:, pl.ds(to, 128)] = part[
                    :, pl.ds(pl.multiple_of(start + g * 128, 128), 128)
                ]


def head_kernel(place, dense, along, result, mine, out, sems, *, sizes):
    rows, block = out.shape[0], dense.shape[2]
    own = along.shape[1]
    at = 0
    for y in range(block // 128):
        for j in range(dense.shape[0]):
            mine[at : at + own, :] = along[j, :, y * 128 : (y + 1) * 128]
            at += own
    numbers = mine[:, rows : rows + 2].astype(jnp.float32)
    ids = (numbers[:, :1] * 256 + numbers[:, 1:]).astype(jnp.int32)
    ids = ids - lax.rem(place[0], sizes[4]) * out.shape[1]
    spots = lax.broadcasted_iota(jnp.int32, (at, block), 1)
    moves = []
    for j in range(dense.shape[0]):
        found = jnp.where(ids - j * block == spots, 1.0, 0.0).astype(jnp.bfloat16)
        made = lax.dot_general(
            mine[:, :rows], found, (((0,), (0,)), ((), ())), preferred_element_type=jnp.float32
        )
        lanes = slice(j * block, (j + 1) * block)
        out[:, lanes] = made + dense[j].astype(jnp.float32)
        moves.append(pltpu.make_async_copy(out.at[:, lanes], result.at[:, lanes], sems.at[j]))
        moves[j].start()
    for move in moves:
        move.wait()


def per_device(hidden, embed_grad, token_ids, loss_weight, teacher_logits, head):
    bf16, f32, f16 = jnp.bfloat16, jnp.float32, jnp.float16
    shape = tuple(lax.axis_size(axis) for axis in DP + ("vocab",))
    nz, nx, ny, nc, nv = shape
    own, width = hidden.shape
    rows, vocab = head.shape
    cols = nz * nx * nc
    block = vocab // cols
    tokens = cols * ny * own
    part = cols * rows
    group = cols * own
    place = lax.axis_index(DP + ("vocab",)).astype(jnp.int32).reshape(1)

    stacked, *pieces = call(
        functools.partial(send_kernel, sizes=shape),
        [held((cols, rows + 2 * own, block), bf16)] + [held((own, 2 * part + 128), bf16)] * ny,
        [pltpu.VMEM((own, width), bf16)] * 2 + [pltpu.SemaphoreType.DMA((2 + 2 * cols,))],
        [SMEM, SMEM, HBM, HBM, HBM, HBM],
    )(place, token_ids, loss_weight, hidden, embed_grad, head, teacher_logits)
    stacked = exchange(stacked, COLS)
    teacher = stacked[:, rows : rows + own].reshape(group, block).astype(f32)
    weights = stacked[:, rows + own :, :: block // 4].reshape(group, 4).astype(f32)
    weights = weights[:, 0] + weights[:, 1] + weights[:, 2] + weights[:, 3]

    line = [pieces[0]] + [shifted(pieces[k], "y", k) for k in range(1, ny)]
    embed_part = jnp.stack([piece[:, part:] for piece in line])
    line = jnp.concatenate([piece[:, :part] for piece in line], axis=0)
    steps = [(dz, dx) for dx in range(nx) for dz in range(nz)][1:]
    same = jnp.concatenate([line] + [shifted_both(line, *step) for step in steps], axis=0)
    other = shifted(same, "c", 1)

    *partials, head_part = call(
        functools.partial(student_kernel, sizes=shape, own=own, rows=rows),
        [held((group, block), f32)] * ny + [stored((part, block), bf16)],
        [pltpu.VMEM((part, block), bf16), pltpu.SemaphoreType.DMA],
    )(place, same, other, stacked)
    student = partials[0]
    for k in range(1, ny):
        student = student + shifted(partials[k], "y", -k)

    along = jnp.concatenate(
        [
            embed_part[:, :, :part].reshape(ny, own, cols, rows),
            jnp.broadcast_to(embed_part[:, :, None, part + rows :], (ny, own, cols, 128 - rows)),
        ],
        axis=3,
    )
    along = along.transpose(2, 1, 0, 3).reshape(cols, own, ny * 128)
    along = exchange(along, COLS)

    student_max = jnp.max(student, axis=1)
    teacher_max = jnp.max(teacher, axis=1)
    student_sum = jnp.sum(jnp.exp(student - student_max[:, None]), axis=1)
    teacher_sum = jnp.sum(jnp.exp(teacher - teacher_max[:, None]), axis=1)
    stats = jnp.stack(
        [student_max + jnp.log(student_sum), teacher_max + jnp.log(teacher_sum)]
    )
    stats = jnp.broadcast_to(stats[None], (cols * nv, *stats.shape))
    stats, along = lax.optimization_barrier((stats, along))
    norms = joined(exchange(stats, COLS + ("vocab",)))
    gap = (
        weights[:, None]
        * (jnp.exp(student - norms[0][:, None]) - jnp.exp(teacher - norms[1][:, None]))
    ).astype(bf16)
    gaps = [gap] + [shifted(gap, "y", k) for k in range(1, ny)]

    half = tokens // nc
    back, back_other, gap_all = call(
        functools.partial(back_kernel, sizes=shape, own=own),
        [held((half, part), f32), held((half, part), f32), held((tokens, block), bf16)],
        [pltpu.VMEM((part, block), bf16), pltpu.SemaphoreType.DMA],
        [VMEM] * ny + [HBM],
    )(place, *gaps, head_part)

    dense = dot(same, gap_all[:half], ((0,), (0,))) + dot(other, gap_all[half:], ((0,), (0,)))
    dense = dense.astype(bf16).reshape(cols, rows, block)

    back = back + shifted(back_other, "c", 1)
    back = back.reshape(nx * nz, ny * own, part)
    sent = (back * FIT).astype(f16)
    came = []
    for k, (dz, dx) in enumerate(steps, 1):
        came.append(shifted_both(sent[k], dz, -dx).astype(f32) * (1 / FIT))
    dense = exchange(dense, COLS)
    total = functools.reduce(jnp.add, came, back[0])
    total = total.reshape(ny, own, part)
    spread = call(
        functools.partial(arrange_kernel, sizes=shape), [held((own, width // nv), f32)] * nv
    )(place, total[0], *[shifted(total[k], "y", -k) for k in range(1, ny)])
    spread = [spread[0]] + [shifted(spread[k], "vocab", k) for k in range(1, nv)]
    head_grad = call(
        functools.partial(head_kernel, sizes=shape),
        [stored((rows, vocab), f32)],
        [pltpu.VMEM((tokens, 128), bf16), pltpu.VMEM((rows, vocab), f32), pltpu.SemaphoreType.DMA((cols,))],
    )(place, dense, along)[0]
    spread, head_grad = lax.optimization_barrier((spread, head_grad))
    grad_hidden = functools.reduce(jnp.add, spread).astype(bf16)
    return grad_hidden, head_grad


def solution(mesh):
    torus = Mesh(
        mesh.devices.reshape(2, 4, 4, 2, mesh.shape["vocab"]), ("z", "x", "y", "c", "vocab")
    )
    in_specs = (P(DP, None), P(DP, None), P(DP), P(DP), P(DP, "vocab"), P(DP, "vocab"))
    out_specs = (P(DP, "vocab"), P(DP, "vocab"))

    return jax.shard_map(
        per_device, mesh=torus, in_specs=in_specs, out_specs=out_specs, check_vma=False
    )
```

```python
import functools

import jax
import jax.numpy as jnp
from jax import lax
from jax.experimental import pallas as pl
from jax.experimental.pallas import tpu as pltpu
from jax.sharding import Mesh
from jax.sharding import PartitionSpec as P


DP = ("z", "x", "y", "c")
COLS = ("z", "x", "c")
FIT = 64.0
SMEM = pl.BlockSpec(memory_space=pltpu.SMEM)
VMEM = pl.BlockSpec(memory_space=pltpu.VMEM)
HBM = pl.BlockSpec(memory_space=pltpu.MemorySpace.HBM)


def exchange(x, axes):
    return lax.all_to_all(x, axes, 0, 0, tiled=True)


def shifted(x, axis, step):
    size = lax.axis_size(axis)
    return lax.ppermute(x, axis, [(k, (k + step) % size) for k in range(size)])


def shifted_both(x, z_step, x_step):
    nz, nx = lax.axis_size("z"), lax.axis_size("x")
    pairs = [
        (z * nx + k, (z + z_step) % nz * nx + (k + x_step) % nx)
        for z in range(nz)
        for k in range(nx)
    ]
    return lax.ppermute(x, ("z", "x"), pairs)


def dot(left, right, contract):
    return lax.dot_general(left, right, (contract, ((), ())), preferred_element_type=jnp.float32)


def call(body, outs, scratch=(), ins=None):
    def run(place, *operands):
        specs = list(ins or [VMEM] * len(operands))
        operands = [
            pltpu.with_memory_space_constraint(x, pltpu.MemorySpace.HBM) if spec is not VMEM else x
            for x, spec in zip(operands, specs)
        ]
        return pl.pallas_call(
            body,
            out_shape=[spec.memory_space(out.shape, out.dtype) for out, spec in outs],
            in_specs=[SMEM] + specs,
            out_specs=[spec for _, spec in outs],
            scratch_shapes=list(scratch),
            compiler_params=pltpu.CompilerParams(vmem_limit_bytes=16 << 20),
        )(place, *operands)

    return run


def held(shape, dtype):
    return jax.ShapeDtypeStruct(shape, dtype), VMEM


def stored(shape, dtype):
    return jax.ShapeDtypeStruct(shape, dtype), HBM


def joined(x):
    top = jnp.max(x, axis=0)
    return top + jnp.log(jnp.sum(jnp.exp(x - top), axis=0))


def position(place, sizes):
    _, nx, ny, nc, nv = sizes
    at = place[0] // nv
    c = lax.rem(at, nc)
    y = lax.rem(at // nc, ny)
    x = lax.rem(at // (nc * ny), nx)
    return at // (nc * ny * nx), x, y, c


def row_of(where, sizes, dc, dx, dz):
    nz, nx, _, nc, _ = sizes
    z = lax.rem(where[0] + (nz - dz), nz)
    x = lax.rem(where[1] + (nx - dx), nx)
    c = lax.rem(where[3] + (nc - dc), nc)
    return (z * nx + x) * nc + c


def send_kernel(place, ids, weights, hidden, embed, head, teacher, *refs, sizes):
    nz, nx, ny, _, _ = sizes
    stacked, outs = refs[0], refs[1 : 1 + ny]
    hidden_here, embed_here, sems = refs[1 + ny :]
    _, _, y, _ = position(place, sizes)
    rows, own = head.shape[0], teacher.shape[0]
    cols, _, block = stacked.shape
    step = hidden.shape[1] // (nz * nx * ny)
    moves = [(hidden, hidden_here), (embed, embed_here)]
    for j in range(cols):
        lanes = slice(j * block, (j + 1) * block)
        moves.append((head.at[:, lanes], stacked.at[j, :rows, :]))
        moves.append((teacher.at[:, lanes], stacked.at[j, rows : rows + own, :]))
    moves = [pltpu.make_async_copy(*move, sems.at[k]) for k, move in enumerate(moves)]
    for move in moves:
        move.start()
    line = lax.broadcasted_iota(jnp.int32, (own, 128), 0)
    lane = lax.broadcasted_iota(jnp.int32, (own, 128), 1)
    weight = jnp.zeros((own, 128), jnp.float32)
    number = jnp.zeros((own, 128), jnp.int32)
    for t in range(own):
        weight = jnp.where(line == t, weights[t], weight)
        number = jnp.where(line == t, ids[t], number)
    number = jnp.where(lane == rows, number // 256, lax.rem(number, 256))
    number = jnp.where((lane == rows) | (lane == rows + 1), number, 0)
    number = number.astype(jnp.float32).astype(jnp.bfloat16)
    for q in range(block // 128):
        piece = weight.astype(jnp.bfloat16)
        weight = weight - piece.astype(jnp.float32)
        for j in range(cols):
            stacked[j, rows + own :, q * 128 : (q + 1) * 128] = piece
    moves[0].wait()
    moves[1].wait()
    for k, out in enumerate(outs):
        to = lax.rem(y + k, ny)
        for g in range(nz * nx):
            lanes = pl.ds(pl.multiple_of((g * ny + to) * step, step), step)
            out[:, g * step : (g + 1) * step] = hidden_here[:, lanes]
            out[:, (nz * nx + g) * step : (nz * nx + g + 1) * step] = embed_here[:, lanes]
        out[:, 2 * nz * nx * step :] = number
    for move in moves[2:]:
        move.wait()


def student_kernel(place, same, other, stacked, *refs, sizes, own, rows):
    where = position(place, sizes)
    nz, nx, ny, nc, _ = sizes
    outs, kept, head, sem = refs[:ny], refs[ny], refs[ny + 1], refs[ny + 2]
    for j in range(nz * nx * nc):
        head[j * rows : (j + 1) * rows, :] = stacked[j, :rows, :]
    keep = pltpu.make_async_copy(head, kept, sem)
    keep.start()
    for dc, half in enumerate((same, other)):
        made = jnp.dot(half[...], head[...], preferred_element_type=jnp.float32)
        at = 0
        for dx in range(nx):
            for dz in range(nz):
                row = pl.multiple_of(row_of(where, sizes, dc, dx, dz) * own, own)
                for k in range(ny):
                    outs[k][pl.ds(row, own), :] = made[at : at + own, :]
                    at += own
    keep.wait()


def back_kernel(place, g0, g1, g2, g3, kept, same, other, gap, head, sem, *, sizes, own):
    where = position(place, sizes)
    nz, nx, _, nc, _ = sizes
    fetch = pltpu.make_async_copy(kept, head, sem)
    fetch.start()
    at = 0
    for dc in range(nc):
        for dx in range(nx):
            for dz in range(nz):
                row = pl.multiple_of(row_of(where, sizes, dc, dx, dz) * own, own)
                for part in (g0, g1, g2, g3):
                    gap[at : at + own, :] = part[pl.ds(row, own), :]
                    at += own
    half = at // nc
    fetch.wait()
    for dc, out in ((1, other), (0, same)):
        out[...] = lax.dot_general(
            gap[dc * half : (dc + 1) * half, :],
            head[...],
            (((1,), (1,)), ((), ())),
            preferred_element_type=jnp.float32,
        )


def arrange_kernel(place, *refs, sizes):
    _, _, ny, _, nv = sizes
    _, _, y, _ = position(place, sizes)
    v = lax.rem(place[0], nv)
    parts, outs = refs[:ny], refs[ny:]
    width = parts[0].shape[1] // nv
    for k, out in enumerate(outs):
        start = lax.rem(v + k, nv) * width
        for j, part in enumerate(parts):
            for g in range(width // 128):
                to = pl.multiple_of((g * ny + lax.rem(y + j, ny)) * 128, 128)
                out[:, pl.ds(to, 128)] = part[
                    :, pl.ds(pl.multiple_of(start + g * 128, 128), 128)
                ]


def embed_kernel(place, along, out, mine, *, sizes):
    rows, block = out.shape[0], along.shape[2]
    own = along.shape[1]
    at = 0
    for y in range(block // 128):
        for j in range(along.shape[0]):
            mine[at : at + own, :] = along[j, :, y * 128 : (y + 1) * 128]
            at += own
    numbers = mine[:, rows : rows + 2].astype(jnp.float32)
    ids = (numbers[:, :1] * 256 + numbers[:, 1:]).astype(jnp.int32)
    ids = ids - lax.rem(place[0], sizes[4]) * out.shape[1]
    spots = lax.broadcasted_iota(jnp.int32, (at, block), 1)
    for j in range(along.shape[0]):
        found = jnp.where(ids - j * block == spots, 1.0, 0.0).astype(jnp.bfloat16)
        out[:, j * block : (j + 1) * block] = lax.dot_general(
            mine[:, :rows], found, (((0,), (0,)), ((), ())), preferred_element_type=jnp.float32
        )


def head_kernel(place, looked, *refs):
    parts, (result, out, sems) = refs[:-3], refs[-3:]
    width = parts[0].shape[2]
    saves = []
    for j in range(parts[0].shape[0]):
        for k, part in enumerate(parts):
            at = (j * len(parts) + k) * width
            lanes = slice(at, at + width)
            out[:, lanes] = looked[:, lanes] + part[j].astype(jnp.float32)
        lanes = slice(j * width * len(parts), (j + 1) * width * len(parts))
        saves.append(pltpu.make_async_copy(out.at[:, lanes], result.at[:, lanes], sems.at[j]))
        saves[j].start()
    for save in saves:
        save.wait()


def per_device(hidden, embed_grad, token_ids, loss_weight, teacher_logits, head):
    bf16, f32, f16 = jnp.bfloat16, jnp.float32, jnp.float16
    shape = tuple(lax.axis_size(axis) for axis in DP + ("vocab",))
    nz, nx, ny, nc, nv = shape
    own, width = hidden.shape
    rows, vocab = head.shape
    cols = nz * nx * nc
    block = vocab // cols
    tokens = cols * ny * own
    part = cols * rows
    group = cols * own
    place = lax.axis_index(DP + ("vocab",)).astype(jnp.int32).reshape(1)

    stacked, *pieces = call(
        functools.partial(send_kernel, sizes=shape),
        [held((cols, rows + 2 * own, block), bf16)] + [held((own, 2 * part + 128), bf16)] * ny,
        [pltpu.VMEM((own, width), bf16)] * 2 + [pltpu.SemaphoreType.DMA((2 + 2 * cols,))],
        [SMEM, SMEM, HBM, HBM, HBM, HBM],
    )(place, token_ids, loss_weight, hidden, embed_grad, head, teacher_logits)
    stacked = exchange(stacked, COLS)
    teacher = stacked[:, rows : rows + own].reshape(group, block).astype(f32)
    weights = stacked[:, rows + own :, :: block // 4].reshape(group, 4).astype(f32)
    weights = weights[:, 0] + weights[:, 1] + weights[:, 2] + weights[:, 3]

    line = [pieces[0]] + [shifted(pieces[k], "y", k) for k in range(1, ny)]
    embed_part = jnp.stack([piece[:, part:] for piece in line])
    line = jnp.concatenate([piece[:, :part] for piece in line], axis=0)
    steps = [(dz, dx) for dx in range(nx) for dz in range(nz)][1:]
    same = jnp.concatenate([line] + [shifted_both(line, *step) for step in steps], axis=0)
    other = shifted(same, "c", 1)

    *partials, head_part = call(
        functools.partial(student_kernel, sizes=shape, own=own, rows=rows),
        [held((group, block), f32)] * ny + [stored((part, block), bf16)],
        [pltpu.VMEM((part, block), bf16), pltpu.SemaphoreType.DMA],
    )(place, same, other, stacked)
    student = partials[0]
    for k in range(1, ny):
        student = student + shifted(partials[k], "y", -k)

    along = jnp.concatenate(
        [
            embed_part[:, :, :part].reshape(ny, own, cols, rows),
            jnp.broadcast_to(embed_part[:, :, None, part + rows :], (ny, own, cols, 128 - rows)),
        ],
        axis=3,
    )
    along = along.transpose(2, 1, 0, 3).reshape(cols, own, ny * 128)
    along = exchange(along, COLS)

    student_max = jnp.max(student, axis=1)
    teacher_max = jnp.max(teacher, axis=1)
    student_sum = jnp.sum(jnp.exp(student - student_max[:, None]), axis=1)
    teacher_sum = jnp.sum(jnp.exp(teacher - teacher_max[:, None]), axis=1)
    stats = jnp.stack(
        [student_max + jnp.log(student_sum), teacher_max + jnp.log(teacher_sum)]
    )
    stats = jnp.broadcast_to(stats[None], (cols * nv, *stats.shape))
    stats, along = lax.optimization_barrier((stats, along))
    norms = joined(exchange(stats, COLS + ("vocab",)))
    gap = (
        weights[:, None]
        * (jnp.exp(student - norms[0][:, None]) - jnp.exp(teacher - norms[1][:, None]))
    ).astype(bf16)
    gaps = [gap] + [shifted(gap, "y", k) for k in range(1, ny)]

    half = tokens // nc
    back, back_other, gap_all = call(
        functools.partial(back_kernel, sizes=shape, own=own),
        [held((half, part), f32), held((half, part), f32), held((tokens, block), bf16)],
        [pltpu.VMEM((part, block), bf16), pltpu.SemaphoreType.DMA],
        [VMEM] * ny + [HBM],
    )(place, *gaps, head_part)

    dense = []
    for k in range(1):
        at = gap_all[:, k * block // 1 : (k + 1) * block // 1]
        made = dot(same, at[:half], ((0,), (0,))) + dot(other, at[half:], ((0,), (0,)))
        dense.append(made.astype(bf16).reshape(cols, rows, block // 1))

    back = back + shifted(back_other, "c", 1)
    back = back.reshape(nx * nz, ny * own, part)
    sent = (back * FIT).astype(f16)
    came = []
    for k, (dz, dx) in enumerate(steps, 1):
        came.append(shifted_both(sent[k], dz, -dx).astype(f32) * (1 / FIT))
    dense[0] = exchange(dense[0], COLS)
    looked = call(
        functools.partial(embed_kernel, sizes=shape),
        [held((rows, vocab), f32)],
        [pltpu.VMEM((tokens, 128), bf16)],
    )(place, along)[0]
    total = functools.reduce(jnp.add, came, back[0])
    total = total.reshape(ny, own, part)
    spread = call(
        functools.partial(arrange_kernel, sizes=shape), [held((own, width // nv), f32)] * nv
    )(place, total[0], *[shifted(total[k], "y", -k) for k in range(1, ny)])
    spread = [spread[0]] + [shifted(spread[k], "vocab", k) for k in range(1, nv)]
    head_grad = call(
        head_kernel,
        [stored((rows, vocab), f32)],
        [pltpu.VMEM((rows, vocab), f32), pltpu.SemaphoreType.DMA((cols,))],
    )(place, looked, *dense)[0]
    spread, head_grad = lax.optimization_barrier((spread, head_grad))
    grad_hidden = functools.reduce(jnp.add, spread).astype(bf16)
    return grad_hidden, head_grad


def solution(mesh):
    torus = Mesh(
        mesh.devices.reshape(2, 4, 4, 2, mesh.shape["vocab"]), ("z", "x", "y", "c", "vocab")
    )
    in_specs = (P(DP, None), P(DP, None), P(DP), P(DP), P(DP, "vocab"), P(DP, "vocab"))
    out_specs = (P(DP, "vocab"), P(DP, "vocab"))

    return jax.shard_map(
        per_device, mesh=torus, in_specs=in_specs, out_specs=out_specs, check_vma=False
    )
```

```python
import functools

import jax
import jax.numpy as jnp
from jax import lax
from jax.experimental import pallas as pl
from jax.experimental.pallas import tpu as pltpu
from jax.sharding import Mesh
from jax.sharding import PartitionSpec as P


DP = ("z", "x", "y", "c")
COLS = ("z", "x", "c")
FIT = 64.0
SMEM = pl.BlockSpec(memory_space=pltpu.SMEM)
VMEM = pl.BlockSpec(memory_space=pltpu.VMEM)
HBM = pl.BlockSpec(memory_space=pltpu.MemorySpace.HBM)


def exchange(x, axes):
    return lax.all_to_all(x, axes, 0, 0, tiled=True)


def shifted(x, axis, step):
    size = lax.axis_size(axis)
    return lax.ppermute(x, axis, [(k, (k + step) % size) for k in range(size)])


def shifted_both(x, z_step, x_step):
    nz, nx = lax.axis_size("z"), lax.axis_size("x")
    pairs = [
        (z * nx + k, (z + z_step) % nz * nx + (k + x_step) % nx)
        for z in range(nz)
        for k in range(nx)
    ]
    return lax.ppermute(x, ("z", "x"), pairs)


def dot(left, right, contract):
    return lax.dot_general(left, right, (contract, ((), ())), preferred_element_type=jnp.float32)


def call(body, outs, scratch=(), ins=None):
    def run(place, *operands):
        specs = list(ins or [VMEM] * len(operands))
        operands = [
            pltpu.with_memory_space_constraint(x, pltpu.MemorySpace.HBM) if spec is not VMEM else x
            for x, spec in zip(operands, specs)
        ]
        return pl.pallas_call(
            body,
            out_shape=[spec.memory_space(out.shape, out.dtype) for out, spec in outs],
            in_specs=[SMEM] + specs,
            out_specs=[spec for _, spec in outs],
            scratch_shapes=list(scratch),
            compiler_params=pltpu.CompilerParams(vmem_limit_bytes=16 << 20),
        )(place, *operands)

    return run


def held(shape, dtype):
    return jax.ShapeDtypeStruct(shape, dtype), VMEM


def stored(shape, dtype):
    return jax.ShapeDtypeStruct(shape, dtype), HBM


def joined(x):
    top = jnp.max(x, axis=0)
    return top + jnp.log(jnp.sum(jnp.exp(x - top), axis=0))


def position(place, sizes):
    _, nx, ny, nc, nv = sizes
    at = place[0] // nv
    c = lax.rem(at, nc)
    y = lax.rem(at // nc, ny)
    x = lax.rem(at // (nc * ny), nx)
    return at // (nc * ny * nx), x, y, c


def row_of(where, sizes, dc, dx, dz):
    nz, nx, _, nc, _ = sizes
    z = lax.rem(where[0] + (nz - dz), nz)
    x = lax.rem(where[1] + (nx - dx), nx)
    c = lax.rem(where[3] + (nc - dc), nc)
    return (z * nx + x) * nc + c


def send_kernel(place, ids, weights, hidden, embed, head, teacher, *refs, sizes):
    nz, nx, ny, _, _ = sizes
    sent, outs = refs[0], refs[1 : 1 + ny]
    hidden_here, embed_here, stacked, sems = refs[1 + ny :]
    _, _, y, _ = position(place, sizes)
    rows, own = head.shape[0], teacher.shape[0]
    cols, _, block = stacked.shape
    step = hidden.shape[1] // (nz * nx * ny)
    moves = [(hidden, hidden_here), (embed, embed_here)]
    for j in range(cols):
        lanes = slice(j * block, (j + 1) * block)
        moves.append((head.at[:, lanes], stacked.at[j, :rows, :]))
        moves.append((teacher.at[:, lanes], stacked.at[j, rows : rows + own, :]))
    moves = [pltpu.make_async_copy(*move, sems.at[k]) for k, move in enumerate(moves)]
    for move in moves:
        move.start()
    line = lax.broadcasted_iota(jnp.int32, (own, 128), 0)
    lane = lax.broadcasted_iota(jnp.int32, (own, 128), 1)
    weight = jnp.zeros((own, 128), jnp.float32)
    number = jnp.zeros((own, 128), jnp.int32)
    for t in range(own):
        weight = jnp.where(line == t, weights[t], weight)
        number = jnp.where(line == t, ids[t], number)
    number = jnp.where(lane == rows, number // 256, lax.rem(number, 256))
    number = jnp.where((lane == rows) | (lane == rows + 1), number, 0)
    number = number.astype(jnp.float32).astype(jnp.bfloat16)
    for q in range(block // 128):
        piece = weight.astype(jnp.bfloat16)
        weight = weight - piece.astype(jnp.float32)
        for j in range(cols):
            stacked[j, rows + own :, q * 128 : (q + 1) * 128] = piece
    saves = []
    for j in range(cols):
        moves[2 + 2 * j].wait()
        moves[3 + 2 * j].wait()
        saves.append(
            pltpu.make_async_copy(stacked.at[j], sent.at[j], sems.at[2 + 2 * cols + j])
        )
        saves[j].start()
    moves[0].wait()
    moves[1].wait()
    for k, out in enumerate(outs):
        to = lax.rem(y + k, ny)
        for g in range(nz * nx):
            lanes = pl.ds(pl.multiple_of((g * ny + to) * step, step), step)
            out[:, g * step : (g + 1) * step] = hidden_here[:, lanes]
            out[:, (nz * nx + g) * step : (nz * nx + g + 1) * step] = embed_here[:, lanes]
        out[:, 2 * nz * nx * step :] = number
    for save in saves:
        save.wait()


def student_kernel(place, same, other, stacked, *refs, sizes, own, rows):
    where = position(place, sizes)
    nz, nx, ny, nc, _ = sizes
    outs, kept, head, sem = refs[:ny], refs[ny], refs[ny + 1], refs[ny + 2]
    for j in range(nz * nx * nc):
        head[j * rows : (j + 1) * rows, :] = stacked[j, :rows, :]
    keep = pltpu.make_async_copy(head, kept, sem)
    keep.start()
    for dc, half in enumerate((same, other)):
        made = jnp.dot(half[...], head[...], preferred_element_type=jnp.float32)
        at = 0
        for dx in range(nx):
            for dz in range(nz):
                row = pl.multiple_of(row_of(where, sizes, dc, dx, dz) * own, own)
                for k in range(ny):
                    outs[k][pl.ds(row, own), :] = made[at : at + own, :]
                    at += own
    keep.wait()


def back_kernel(place, g0, g1, g2, g3, kept, same, other, gap, head, sem, *, sizes, own):
    where = position(place, sizes)
    nz, nx, _, nc, _ = sizes
    fetch = pltpu.make_async_copy(kept, head, sem)
    fetch.start()
    at = 0
    for dc in range(nc):
        for dx in range(nx):
            for dz in range(nz):
                row = pl.multiple_of(row_of(where, sizes, dc, dx, dz) * own, own)
                for part in (g0, g1, g2, g3):
                    gap[at : at + own, :] = part[pl.ds(row, own), :]
                    at += own
    half = at // nc
    fetch.wait()
    for dc, out in ((1, other), (0, same)):
        out[...] = lax.dot_general(
            gap[dc * half : (dc + 1) * half, :],
            head[...],
            (((1,), (1,)), ((), ())),
            preferred_element_type=jnp.float32,
        )


def arrange_kernel(place, *refs, sizes):
    _, _, ny, _, nv = sizes
    _, _, y, _ = position(place, sizes)
    v = lax.rem(place[0], nv)
    parts, outs = refs[:ny], refs[ny:]
    width = parts[0].shape[1] // nv
    for k, out in enumerate(outs):
        start = lax.rem(v + k, nv) * width
        for j, part in enumerate(parts):
            for g in range(width // 128):
                to = pl.multiple_of((g * ny + lax.rem(y + j, ny)) * 128, 128)
                out[:, pl.ds(to, 128)] = part[
                    :, pl.ds(pl.multiple_of(start + g * 128, 128), 128)
                ]


def embed_kernel(place, along, out, mine, *, sizes):
    rows, block = out.shape[0], along.shape[2]
    own = along.shape[1]
    at = 0
    for y in range(block // 128):
        for j in range(along.shape[0]):
            mine[at : at + own, :] = along[j, :, y * 128 : (y + 1) * 128]
            at += own
    numbers = mine[:, rows : rows + 2].astype(jnp.float32)
    ids = (numbers[:, :1] * 256 + numbers[:, 1:]).astype(jnp.int32)
    ids = ids - lax.rem(place[0], sizes[4]) * out.shape[1]
    spots = lax.broadcasted_iota(jnp.int32, (at, block), 1)
    for j in range(along.shape[0]):
        found = jnp.where(ids - j * block == spots, 1.0, 0.0).astype(jnp.bfloat16)
        out[:, j * block : (j + 1) * block] = lax.dot_general(
            mine[:, :rows], found, (((0,), (0,)), ((), ())), preferred_element_type=jnp.float32
        )


def head_kernel(place, looked, *refs):
    parts, (result, out, sems) = refs[:-3], refs[-3:]
    width = parts[0].shape[2]
    saves = []
    for j in range(parts[0].shape[0]):
        for k, part in enumerate(parts):
            at = (j * len(parts) + k) * width
            lanes = slice(at, at + width)
            out[:, lanes] = looked[:, lanes] + part[j].astype(jnp.float32)
        lanes = slice(j * width * len(parts), (j + 1) * width * len(parts))
        saves.append(pltpu.make_async_copy(out.at[:, lanes], result.at[:, lanes], sems.at[j]))
        saves[j].start()
    for save in saves:
        save.wait()


def per_device(hidden, embed_grad, token_ids, loss_weight, teacher_logits, head):
    bf16, f32, f16 = jnp.bfloat16, jnp.float32, jnp.float16
    shape = tuple(lax.axis_size(axis) for axis in DP + ("vocab",))
    nz, nx, ny, nc, nv = shape
    own, width = hidden.shape
    rows, vocab = head.shape
    cols = nz * nx * nc
    block = vocab // cols
    tokens = cols * ny * own
    part = cols * rows
    group = cols * own
    place = lax.axis_index(DP + ("vocab",)).astype(jnp.int32).reshape(1)

    stacked, *pieces = call(
        functools.partial(send_kernel, sizes=shape),
        [stored((cols, rows + 2 * own, block), bf16)] + [held((own, 2 * part + 128), bf16)] * ny,
        [pltpu.VMEM((own, width), bf16)] * 2
        + [
            pltpu.VMEM((cols, rows + 2 * own, block), bf16),
            pltpu.SemaphoreType.DMA((2 + 3 * cols,)),
        ],
        [SMEM, SMEM, HBM, HBM, HBM, HBM],
    )(place, token_ids, loss_weight, hidden, embed_grad, head, teacher_logits)
    stacked = exchange(stacked, COLS)
    teacher = stacked[:, rows : rows + own].reshape(group, block).astype(f32)
    weights = stacked[:, rows + own :, :: block // 4].reshape(group, 4).astype(f32)
    weights = weights[:, 0] + weights[:, 1] + weights[:, 2] + weights[:, 3]

    line = [pieces[0]] + [shifted(pieces[k], "y", k) for k in range(1, ny)]
    embed_part = jnp.stack([piece[:, part:] for piece in line])
    line = jnp.concatenate([piece[:, :part] for piece in line], axis=0)
    steps = [(dz, dx) for dx in range(nx) for dz in range(nz)][1:]
    same = jnp.concatenate([line] + [shifted_both(line, *step) for step in steps], axis=0)
    other = shifted(same, "c", 1)

    *partials, head_part = call(
        functools.partial(student_kernel, sizes=shape, own=own, rows=rows),
        [held((group, block), f32)] * ny + [stored((part, block), bf16)],
        [pltpu.VMEM((part, block), bf16), pltpu.SemaphoreType.DMA],
    )(place, same, other, stacked)
    student = partials[0]
    for k in range(1, ny):
        student = student + shifted(partials[k], "y", -k)

    along = jnp.concatenate(
        [
            embed_part[:, :, :part].reshape(ny, own, cols, rows),
            jnp.broadcast_to(embed_part[:, :, None, part + rows :], (ny, own, cols, 128 - rows)),
        ],
        axis=3,
    )
    along = along.transpose(2, 1, 0, 3).reshape(cols, own, ny * 128)
    along = exchange(along, COLS)

    student_max = jnp.max(student, axis=1)
    teacher_max = jnp.max(teacher, axis=1)
    student_sum = jnp.sum(jnp.exp(student - student_max[:, None]), axis=1)
    teacher_sum = jnp.sum(jnp.exp(teacher - teacher_max[:, None]), axis=1)
    stats = jnp.stack(
        [student_max + jnp.log(student_sum), teacher_max + jnp.log(teacher_sum)]
    )
    stats = jnp.broadcast_to(stats[None], (cols * nv, *stats.shape))
    stats, along = lax.optimization_barrier((stats, along))
    norms = joined(exchange(stats, COLS + ("vocab",)))
    gap = (
        weights[:, None]
        * (jnp.exp(student - norms[0][:, None]) - jnp.exp(teacher - norms[1][:, None]))
    ).astype(bf16)
    gaps = [gap] + [shifted(gap, "y", k) for k in range(1, ny)]

    half = tokens // nc
    back, back_other, gap_all = call(
        functools.partial(back_kernel, sizes=shape, own=own),
        [held((half, part), f32), held((half, part), f32), held((tokens, block), bf16)],
        [pltpu.VMEM((part, block), bf16), pltpu.SemaphoreType.DMA],
        [VMEM] * ny + [HBM],
    )(place, *gaps, head_part)

    dense = []
    for k in range(1):
        at = gap_all[:, k * block // 1 : (k + 1) * block // 1]
        made = dot(same, at[:half], ((0,), (0,))) + dot(other, at[half:], ((0,), (0,)))
        dense.append(made.astype(bf16).reshape(cols, rows, block // 1))

    back = back + shifted(back_other, "c", 1)
    back = back.reshape(nx * nz, ny * own, part)
    sent = (back * FIT).astype(f16)
    came = []
    for k, (dz, dx) in enumerate(steps, 1):
        came.append(shifted_both(sent[k], dz, -dx).astype(f32) * (1 / FIT))
    dense[0] = exchange(dense[0], COLS)
    looked = call(
        functools.partial(embed_kernel, sizes=shape),
        [held((rows, vocab), f32)],
        [pltpu.VMEM((tokens, 128), bf16)],
    )(place, along)[0]
    total = functools.reduce(jnp.add, came, back[0])
    total = total.reshape(ny, own, part)
    spread = call(
        functools.partial(arrange_kernel, sizes=shape), [held((own, width // nv), f32)] * nv
    )(place, total[0], *[shifted(total[k], "y", -k) for k in range(1, ny)])
    spread = [spread[0]] + [shifted(spread[k], "vocab", k) for k in range(1, nv)]
    head_grad = call(
        head_kernel,
        [stored((rows, vocab), f32)],
        [pltpu.VMEM((rows, vocab), f32), pltpu.SemaphoreType.DMA((cols,))],
    )(place, looked, *dense)[0]
    spread, head_grad = lax.optimization_barrier((spread, head_grad))
    grad_hidden = functools.reduce(jnp.add, spread).astype(bf16)
    return grad_hidden, head_grad


def solution(mesh):
    torus = Mesh(
        mesh.devices.reshape(2, 4, 4, 2, mesh.shape["vocab"]), ("z", "x", "y", "c", "vocab")
    )
    in_specs = (P(DP, None), P(DP, None), P(DP), P(DP), P(DP, "vocab"), P(DP, "vocab"))
    out_specs = (P(DP, "vocab"), P(DP, "vocab"))

    return jax.shard_map(
        per_device, mesh=torus, in_specs=in_specs, out_specs=out_specs, check_vma=False
    )
```

```python
import functools

import jax
import jax.numpy as jnp
from jax import lax
from jax.experimental import pallas as pl
from jax.experimental.pallas import tpu as pltpu
from jax.sharding import Mesh
from jax.sharding import PartitionSpec as P


DP = ("z", "x", "y", "c")
COLS = ("z", "x", "c")
FIT = 64.0
SMEM = pl.BlockSpec(memory_space=pltpu.SMEM)
VMEM = pl.BlockSpec(memory_space=pltpu.VMEM)
HBM = pl.BlockSpec(memory_space=pltpu.MemorySpace.HBM)


def exchange(x, axes):
    return lax.all_to_all(x, axes, 0, 0, tiled=True)


def shifted(x, axis, step):
    size = lax.axis_size(axis)
    return lax.ppermute(x, axis, [(k, (k + step) % size) for k in range(size)])


def shifted_both(x, z_step, x_step):
    nz, nx = lax.axis_size("z"), lax.axis_size("x")
    pairs = [
        (z * nx + k, (z + z_step) % nz * nx + (k + x_step) % nx)
        for z in range(nz)
        for k in range(nx)
    ]
    return lax.ppermute(x, ("z", "x"), pairs)


def dot(left, right, contract):
    return lax.dot_general(left, right, (contract, ((), ())), preferred_element_type=jnp.float32)


def call(body, outs, scratch=(), ins=None):
    def run(place, *operands):
        specs = list(ins or [VMEM] * len(operands))
        operands = [
            pltpu.with_memory_space_constraint(x, pltpu.MemorySpace.HBM) if spec is not VMEM else x
            for x, spec in zip(operands, specs)
        ]
        return pl.pallas_call(
            body,
            out_shape=[spec.memory_space(out.shape, out.dtype) for out, spec in outs],
            in_specs=[SMEM] + specs,
            out_specs=[spec for _, spec in outs],
            scratch_shapes=list(scratch),
            compiler_params=pltpu.CompilerParams(vmem_limit_bytes=16 << 20),
        )(place, *operands)

    return run


def held(shape, dtype):
    return jax.ShapeDtypeStruct(shape, dtype), VMEM


def stored(shape, dtype):
    return jax.ShapeDtypeStruct(shape, dtype), HBM


def joined(x):
    top = jnp.max(x, axis=0)
    return top + jnp.log(jnp.sum(jnp.exp(x - top), axis=0))


def position(place, sizes):
    _, nx, ny, nc, nv = sizes
    at = place[0] // nv
    c = lax.rem(at, nc)
    y = lax.rem(at // nc, ny)
    x = lax.rem(at // (nc * ny), nx)
    return at // (nc * ny * nx), x, y, c


def row_of(where, sizes, dc, dx, dz):
    nz, nx, _, nc, _ = sizes
    z = lax.rem(where[0] + (nz - dz), nz)
    x = lax.rem(where[1] + (nx - dx), nx)
    c = lax.rem(where[3] + (nc - dc), nc)
    return (z * nx + x) * nc + c


def send_kernel(place, ids, weights, hidden, embed, head, teacher, *refs, sizes):
    nz, nx, ny, _, _ = sizes
    stacked, outs = refs[0], refs[1 : 1 + ny]
    hidden_here, embed_here, sems = refs[1 + ny :]
    _, _, y, _ = position(place, sizes)
    rows, own = head.shape[0], teacher.shape[0]
    cols, _, block = stacked.shape
    step = hidden.shape[1] // (nz * nx * ny)
    moves = [(hidden, hidden_here), (embed, embed_here)]
    for j in range(cols):
        lanes = slice(j * block, (j + 1) * block)
        moves.append((head.at[:, lanes], stacked.at[j, :rows, :]))
        moves.append((teacher.at[:, lanes], stacked.at[j, rows : rows + own, :]))
    moves = [pltpu.make_async_copy(*move, sems.at[k]) for k, move in enumerate(moves)]
    for move in moves:
        move.start()
    line = lax.broadcasted_iota(jnp.int32, (own, 128), 0)
    lane = lax.broadcasted_iota(jnp.int32, (own, 128), 1)
    weight = jnp.zeros((own, 128), jnp.float32)
    number = jnp.zeros((own, 128), jnp.int32)
    for t in range(own):
        weight = jnp.where(line == t, weights[t], weight)
        number = jnp.where(line == t, ids[t], number)
    number = jnp.where(lane == rows, number // 256, lax.rem(number, 256))
    number = jnp.where((lane == rows) | (lane == rows + 1), number, 0)
    number = number.astype(jnp.float32)
    for q in range(4):
        piece = weight.astype(jnp.bfloat16)
        weight = weight - piece.astype(jnp.float32)
        number = jnp.where(lane == rows + 2 + q, piece.astype(jnp.float32), number)
    number = number.astype(jnp.bfloat16)
    moves[0].wait()
    moves[1].wait()
    for k, out in enumerate(outs):
        to = lax.rem(y + k, ny)
        for g in range(nz * nx):
            lanes = pl.ds(pl.multiple_of((g * ny + to) * step, step), step)
            out[:, g * step : (g + 1) * step] = hidden_here[:, lanes]
            out[:, (nz * nx + g) * step : (nz * nx + g + 1) * step] = embed_here[:, lanes]
        out[:, 2 * nz * nx * step :] = number
    for move in moves[2:]:
        move.wait()


def student_kernel(place, same, other, stacked, *refs, sizes, own, rows):
    where = position(place, sizes)
    nz, nx, ny, nc, _ = sizes
    outs, kept, head, sem = refs[:ny], refs[ny], refs[ny + 1], refs[ny + 2]
    for j in range(nz * nx * nc):
        head[j * rows : (j + 1) * rows, :] = stacked[j, :rows, :]
    keep = pltpu.make_async_copy(head, kept, sem)
    keep.start()
    for dc, half in enumerate((same, other)):
        made = jnp.dot(half[...], head[...], preferred_element_type=jnp.float32)
        at = 0
        for dx in range(nx):
            for dz in range(nz):
                row = pl.multiple_of(row_of(where, sizes, dc, dx, dz) * own, own)
                for k in range(ny):
                    outs[k][pl.ds(row, own), :] = made[at : at + own, :]
                    at += own
    keep.wait()


def back_kernel(place, g0, g1, g2, g3, kept, same, other, gap, head, sem, *, sizes, own):
    where = position(place, sizes)
    nz, nx, _, nc, _ = sizes
    fetch = pltpu.make_async_copy(kept, head, sem)
    fetch.start()
    at = 0
    for dc in range(nc):
        for dx in range(nx):
            for dz in range(nz):
                row = pl.multiple_of(row_of(where, sizes, dc, dx, dz) * own, own)
                for part in (g0, g1, g2, g3):
                    gap[at : at + own, :] = part[pl.ds(row, own), :]
                    at += own
    half = at // nc
    fetch.wait()
    for dc, out in ((1, other), (0, same)):
        out[...] = lax.dot_general(
            gap[dc * half : (dc + 1) * half, :],
            head[...],
            (((1,), (1,)), ((), ())),
            preferred_element_type=jnp.float32,
        )


def arrange_kernel(place, *refs, sizes):
    _, _, ny, _, nv = sizes
    _, _, y, _ = position(place, sizes)
    v = lax.rem(place[0], nv)
    parts, outs = refs[:ny], refs[ny:]
    width = parts[0].shape[1] // nv
    for k, out in enumerate(outs):
        start = lax.rem(v + k, nv) * width
        for j, part in enumerate(parts):
            for g in range(width // 128):
                to = pl.multiple_of((g * ny + lax.rem(y + j, ny)) * 128, 128)
                out[:, pl.ds(to, 128)] = part[
                    :, pl.ds(pl.multiple_of(start + g * 128, 128), 128)
                ]


def embed_kernel(place, along, out, mine, *, sizes):
    rows, block = out.shape[0], along.shape[2]
    own = along.shape[1]
    at = 0
    for y in range(block // 128):
        for j in range(along.shape[0]):
            mine[at : at + own, :] = along[j, :, y * 128 : (y + 1) * 128]
            at += own
    numbers = mine[:, rows : rows + 2].astype(jnp.float32)
    ids = (numbers[:, :1] * 256 + numbers[:, 1:]).astype(jnp.int32)
    ids = ids - lax.rem(place[0], sizes[4]) * out.shape[1]
    spots = lax.broadcasted_iota(jnp.int32, (at, block), 1)
    for j in range(along.shape[0]):
        found = jnp.where(ids - j * block == spots, 1.0, 0.0).astype(jnp.bfloat16)
        out[:, j * block : (j + 1) * block] = lax.dot_general(
            mine[:, :rows], found, (((0,), (0,)), ((), ())), preferred_element_type=jnp.float32
        )


def head_kernel(place, looked, *refs):
    parts, (result, out, sems) = refs[:-3], refs[-3:]
    width = parts[0].shape[2]
    saves = []
    for j in range(parts[0].shape[0]):
        for k, part in enumerate(parts):
            at = (j * len(parts) + k) * width
            lanes = slice(at, at + width)
            out[:, lanes] = looked[:, lanes] + part[j].astype(jnp.float32)
        lanes = slice(j * width * len(parts), (j + 1) * width * len(parts))
        saves.append(pltpu.make_async_copy(out.at[:, lanes], result.at[:, lanes], sems.at[j]))
        saves[j].start()
    for save in saves:
        save.wait()


def per_device(hidden, embed_grad, token_ids, loss_weight, teacher_logits, head):
    bf16, f32, f16 = jnp.bfloat16, jnp.float32, jnp.float16
    shape = tuple(lax.axis_size(axis) for axis in DP + ("vocab",))
    nz, nx, ny, nc, nv = shape
    own, width = hidden.shape
    rows, vocab = head.shape
    cols = nz * nx * nc
    block = vocab // cols
    tokens = cols * ny * own
    part = cols * rows
    group = cols * own
    place = lax.axis_index(DP + ("vocab",)).astype(jnp.int32).reshape(1)

    stacked, *pieces = call(
        functools.partial(send_kernel, sizes=shape),
        [held((cols, rows + own, block), bf16)] + [held((own, 2 * part + 128), bf16)] * ny,
        [pltpu.VMEM((own, width), bf16)] * 2 + [pltpu.SemaphoreType.DMA((2 + 2 * cols,))],
        [SMEM, SMEM, HBM, HBM, HBM, HBM],
    )(place, token_ids, loss_weight, hidden, embed_grad, head, teacher_logits)
    stacked = exchange(stacked, COLS)
    teacher = stacked[:, rows : rows + own].reshape(group, block).astype(f32)

    line = [pieces[0]] + [shifted(pieces[k], "y", k) for k in range(1, ny)]
    embed_part = jnp.stack([piece[:, part:] for piece in line])
    line = jnp.concatenate([piece[:, :part] for piece in line], axis=0)
    steps = [(dz, dx) for dx in range(nx) for dz in range(nz)][1:]
    same = jnp.concatenate([line] + [shifted_both(line, *step) for step in steps], axis=0)
    other = shifted(same, "c", 1)

    *partials, head_part = call(
        functools.partial(student_kernel, sizes=shape, own=own, rows=rows),
        [held((group, block), f32)] * ny + [stored((part, block), bf16)],
        [pltpu.VMEM((part, block), bf16), pltpu.SemaphoreType.DMA],
    )(place, same, other, stacked)
    student = partials[0]
    for k in range(1, ny):
        student = student + shifted(partials[k], "y", -k)

    along = jnp.concatenate(
        [
            embed_part[:, :, :part].reshape(ny, own, cols, rows),
            jnp.broadcast_to(embed_part[:, :, None, part + rows :], (ny, own, cols, 128 - rows)),
        ],
        axis=3,
    )
    along = along.transpose(2, 1, 0, 3).reshape(cols, own, ny * 128)
    along = exchange(along, COLS)

    student_max = jnp.max(student, axis=1)
    teacher_max = jnp.max(teacher, axis=1)
    student_sum = jnp.sum(jnp.exp(student - student_max[:, None]), axis=1)
    teacher_sum = jnp.sum(jnp.exp(teacher - teacher_max[:, None]), axis=1)
    stats = jnp.stack(
        [student_max + jnp.log(student_sum), teacher_max + jnp.log(teacher_sum)]
    )
    stats = jnp.broadcast_to(stats[None], (cols * nv, *stats.shape))
    stats, along = lax.optimization_barrier((stats, along))
    weights = along[:, :, rows + 2 : rows + 6].reshape(group, 4).astype(f32)
    weights = weights[:, 0] + weights[:, 1] + weights[:, 2] + weights[:, 3]
    norms = joined(exchange(stats, COLS + ("vocab",)))
    gap = (
        weights[:, None]
        * (jnp.exp(student - norms[0][:, None]) - jnp.exp(teacher - norms[1][:, None]))
    ).astype(bf16)
    gaps = [gap] + [shifted(gap, "y", k) for k in range(1, ny)]

    half = tokens // nc
    back, back_other, gap_all = call(
        functools.partial(back_kernel, sizes=shape, own=own),
        [held((half, part), f32), held((half, part), f32), held((tokens, block), bf16)],
        [pltpu.VMEM((part, block), bf16), pltpu.SemaphoreType.DMA],
        [VMEM] * ny + [HBM],
    )(place, *gaps, head_part)

    dense = []
    for k in range(1):
        at = gap_all[:, k * block // 1 : (k + 1) * block // 1]
        made = dot(same, at[:half], ((0,), (0,))) + dot(other, at[half:], ((0,), (0,)))
        dense.append(made.astype(bf16).reshape(cols, rows, block // 1))

    back = back + shifted(back_other, "c", 1)
    back = back.reshape(nx * nz, ny * own, part)
    sent = (back * FIT).astype(f16)
    came = []
    for k, (dz, dx) in enumerate(steps, 1):
        came.append(shifted_both(sent[k], dz, -dx).astype(f32) * (1 / FIT))
    dense[0] = exchange(dense[0], COLS)
    looked = call(
        functools.partial(embed_kernel, sizes=shape),
        [held((rows, vocab), f32)],
        [pltpu.VMEM((tokens, 128), bf16)],
    )(place, along)[0]
    total = functools.reduce(jnp.add, came, back[0])
    total = total.reshape(ny, own, part)
    spread = call(
        functools.partial(arrange_kernel, sizes=shape), [held((own, width // nv), f32)] * nv
    )(place, total[0], *[shifted(total[k], "y", -k) for k in range(1, ny)])
    spread = [spread[0]] + [shifted(spread[k], "vocab", k) for k in range(1, nv)]
    head_grad = call(
        head_kernel,
        [stored((rows, vocab), f32)],
        [pltpu.VMEM((rows, vocab), f32), pltpu.SemaphoreType.DMA((cols,))],
    )(place, looked, *dense)[0]
    spread, head_grad = lax.optimization_barrier((spread, head_grad))
    grad_hidden = functools.reduce(jnp.add, spread).astype(bf16)
    return grad_hidden, head_grad


def solution(mesh):
    torus = Mesh(
        mesh.devices.reshape(2, 4, 4, 2, mesh.shape["vocab"]), ("z", "x", "y", "c", "vocab")
    )
    in_specs = (P(DP, None), P(DP, None), P(DP), P(DP), P(DP, "vocab"), P(DP, "vocab"))
    out_specs = (P(DP, "vocab"), P(DP, "vocab"))

    return jax.shard_map(
        per_device, mesh=torus, in_specs=in_specs, out_specs=out_specs, check_vma=False
    )
```
